128 devices in a mesh: coarse: 2 (over z_hi), fine: 8 (over z_lo, y), model: 8 (over x, core).
Axes of the slice: x: 4, y: 4, z: 4 (z_hi: 2, z_lo: 2; z = z_hi * 2 + z_lo), core: 2. Of those that a mesh axis runs over, the one named last changes fastest.
Arguments:
- fresh_keys: bfloat16 [16, 24576, 8, 128], P(None, ('coarse', 'fine'), 'model'), may hold values from -6 to 6
- fresh_values: bfloat16 [16, 24576, 8, 128], P(None, ('coarse', 'fine'), 'model'), may hold values from -6 to 6
- turn_angle: float32 [24576, 64], replicated, may hold values from -3.140625 to 3.140625
Outputs:
- cache_keys: bfloat16 [16, 24576, 8, 128], P(('coarse', 'fine'), None, 'model')
- cache_values: bfloat16 [16, 24576, 8, 128], P(('coarse', 'fine'), None, 'model')
- page_high: bfloat16 [16, 768, 8, 128], P(('coarse', 'fine'), None, 'model')
- page_low: bfloat16 [16, 768, 8, 128], P(('coarse', 'fine'), None, 'model')
The draws below stay inside these ranges and needn't reach their ends.
All inputs are finite; a program needn't handle non-finite values.
Results may differ from the reference program's by a relative error of at most 0.001.
Values may be sent and summed in bfloat16 or wider, within the bound.
A program may use at most 128 MiB of HBM per device.

```python
import jax
import jax.numpy as jnp

BATCH = 16
LENGTH = 24576
KV_HEADS = 8
HEAD_SIZE = 128
HALF_HEAD = 64
PAGE = 32


def block_levels(rng, shape, shards, least, largest):
    def one(dim, blocks):
        heights = jax.random.uniform(jax.random.fold_in(jax.random.fold_in(rng, 6), dim), (blocks,), jnp.float32, least / len(shards), largest / len(shards))
        return jnp.repeat(jnp.exp(heights), shape[dim] // blocks).reshape((-1,) + (1,) * (len(shape) - dim - 1))

    factor_of = one(*shards[0])
    for cut in shards[1:]:
        factor_of = factor_of * one(*cut)
    return factor_of


def normal_values(key, dims, width, reach, split=(), kind=jnp.bfloat16):
    array = jax.random.normal(key, dims, jnp.float32) * width
    if len(split) > 0:
        array = block_levels(key, dims, split, -0.22, 0.18) * array
    return jnp.clip(array, min=-reach, max=reach).astype(kind)


def setup_inputs(seed: int = 0) -> dict:
    streams_of = jax.random.split(jax.random.key(seed), 4)
    fresh_keys = normal_values(streams_of[0], (BATCH, LENGTH, KV_HEADS, HEAD_SIZE), 1.0, 6.0, ((1, 16), (2, 8)))
    fresh_values = normal_values(streams_of[1], (BATCH, LENGTH, KV_HEADS, HEAD_SIZE), 1.0, 6.0, ((1, 16), (2, 8)))
    turn_angle = jnp.clip(jax.random.uniform(streams_of[2], (LENGTH, HALF_HEAD), jnp.float32, -3.140625, 3.140625), -3.140625, 3.140625)
    return {"fresh_keys": fresh_keys, "fresh_values": fresh_values, "turn_angle": turn_angle}


def turn_pairs(vectors, angle):
    half = vectors.shape[-1] // 2
    cosine, sine = jnp.cos(angle)[None, :, None, :], jnp.sin(angle)[None, :, None, :]
    first, second = vectors[..., :half], vectors[..., half:]
    return jnp.concatenate([first * cosine - second * sine, second * cosine + first * sine], axis=-1)


def prepare_keys(plain_keys, angle):
    wide_keys = plain_keys.astype(jnp.float32)
    return turn_pairs(wide_keys, angle)


def reference(fresh_keys, fresh_values, turn_angle):
    turned_keys = prepare_keys(fresh_keys, turn_angle)
    narrow_keys = turned_keys.astype(jnp.bfloat16)
    page_view = narrow_keys.reshape(BATCH, LENGTH // PAGE, PAGE, KV_HEADS, HEAD_SIZE)
    page_high = jnp.max(page_view, axis=2)
    page_low = jnp.min(page_view, axis=2)
    cache_keys = narrow_keys
    cache_values = fresh_values
    return cache_keys, cache_values, page_high, page_low
```

```python
import jax
import jax.numpy as jnp
from jax import lax
from jax.experimental import pallas as pl
from jax.experimental.pallas import tpu as pltpu
from jax.sharding import PartitionSpec as P

PAGE = 32
SIDE = 4
MESH = pl.DeviceIdType.MESH
FAR_FIRST = (2, 1, 3)


def exchange(keys, values, angles, key_out, value_out, high_out, low_out, raw, turned, relay, angle, cosine, sine,
             tops, bottoms, send_sem, recv_sem, raw_sem, own_sem, angle_sem):
    length = keys.shape[1]
    half = length // 2
    coarse, fine, model = (lax.axis_index(name) for name in ("coarse", "fine", "model"))
    z, y = coarse * 2 + fine // SIDE, fine % SIDE
    me = z * SIDE + y

    def place(dz, dy):
        return (z + dz) % SIDE * SIDE + (y + dy) % SIDE

    def device(dz, dy):
        pz, py = (z + dz) % SIDE, (y + dy) % SIDE
        return (pz // 2, pz % 2 * SIDE + py, model)

    sources = (values, turned)
    outs = (value_out, key_out)

    def ring(way, step):
        return (0, step) if way == 0 else (step, 0)

    def both(way, first, second):
        return (second, first) if way == 0 else (first, second)

    def hop(item, way, leg, first, second):
        rows = pl.ds(way * half, half)
        at = place(*both(way, first, second))
        if leg == 0:
            src = sources[item].at[at, rows]
            if second == 0:
                dst = outs[item].at[me, rows]
            else:
                dst = relay.at[item, way, first - 1, second - 1]
            to = device(*ring(way, first))
        else:
            if first == 0:
                src = sources[item].at[at, rows]
                origin = me
            else:
                src = relay.at[item, way, first - 1, second - 1]
                origin = place(*both(way, -first, 0))
            dst = outs[item].at[origin, rows]
            to = device(*ring(1 - way, second))
        index = ((item * 2 + way) * 2 + leg) * 16 + first * 4 + second
        return pltpu.make_async_remote_copy(
            src_ref=src, dst_ref=dst, send_sem=send_sem.at[index], recv_sem=recv_sem.at[index],
            device_id=to, device_id_type=MESH,
        )

    barrier = pltpu.get_barrier_semaphore()
    for step in (1, 3, 2):
        for way in (0, 1):
            pl.semaphore_signal(barrier, inc=1, device_id=device(*ring(way, step)), device_id_type=MESH)

    columns = pl.ds(pl.multiple_of(me * length, 128), length)
    angle_copy = pltpu.make_async_copy(angles.at[:, columns], angle, angle_sem)
    angle_copy.start()
    raw_copy = [pltpu.make_async_copy(keys.at[b], raw.at[b], raw_sem.at[b]) for b in range(16)]
    for copy in raw_copy:
        copy.start()
    pl.semaphore_wait(barrier, 6)

    started = []

    def start(*which):
        copy = hop(*which)
        copy.start()
        started.append(copy)

    def leave(item):
        for second in (1, 2, 3, 0):
            for first in FAR_FIRST:
                for way in (0, 1):
                    start(item, way, 0, first, second)

    def forward(item):
        for first in (0, 2, 1, 3):
            for second in FAR_FIRST:
                for way in (0, 1):
                    if first:
                        hop(item, way, 0, first, second).wait_recv()
                    start(item, way, 1, first, second)

    leave(0)
    own_value = pltpu.make_async_copy(values.at[me], value_out.at[me], own_sem.at[0])
    own_value.start()

    angle_copy.wait()
    for at in range(0, length, 128):
        block = angle[:, at:at + 128]
        c, s = jnp.cos(block), jnp.sin(block)
        cosine[at:at + 128, :] = jnp.concatenate([c, c], axis=0).T
        sine[at:at + 128, :] = jnp.concatenate([-s, s], axis=0).T

    def turn(b, _):
        pltpu.make_async_copy(keys.at[b], raw.at[b], raw_sem.at[b]).wait()

        def tile(i, _):
            rows = pl.ds(pl.multiple_of(i * 128, 128), 128)
            x = raw[b, rows, :].astype(jnp.float32)
            turned[b, rows, :] = (x * cosine[rows, :] + pltpu.roll(x, 64, 1) * sine[rows, :]).astype(jnp.bfloat16)
            return 0

        return lax.fori_loop(0, length // 128, tile, 0)

    lax.fori_loop(0, 16, turn, 0)
    leave(1)
    own_key = pltpu.make_async_copy(turned.at[me], key_out.at[me], own_sem.at[1])
    own_key.start()
    forward(0)
    forward(1)

    pages = half // PAGE

    def bounds(origin, way):
        base = origin * (2 * pages) + way * pages

        def group(i, _):
            x = key_out[origin, pl.ds(pl.multiple_of(way * half + i * 8 * PAGE, 8 * PAGE), 8 * PAGE), :]
            x = x.astype(jnp.float32).reshape(8, PAGE, x.shape[-1])
            rows = pl.ds(pl.multiple_of(base + i * 8, 8), 8)
            tops[rows, :] = jnp.max(x, axis=1)
            bottoms[rows, :] = jnp.min(x, axis=1)
            return 0

        lax.fori_loop(0, pages // 8, group, 0)

    own_key.wait()
    for way in (0, 1):
        bounds(me, way)
    for first in FAR_FIRST:
        for way in (0, 1):
            hop(1, way, 0, first, 0).wait_recv()
            bounds(place(*both(way, -first, 0)), way)
    for first in (0, 2, 1, 3):
        for second in FAR_FIRST:
            for way in (0, 1):
                hop(1, way, 1, first, second).wait_recv()
                bounds(place(*both(way, -first, -second)), way)
    high_out[...] = tops[...].astype(jnp.bfloat16)
    low_out[...] = bottoms[...].astype(jnp.bfloat16)
    own_value.wait()
    for way in (0, 1):
        for first in FAR_FIRST:
            hop(0, way, 0, first, 0).wait_recv()
        for first in range(4):
            for second in FAR_FIRST:
                hop(0, way, 1, first, second).wait_recv()
    for copy in started:
        copy.wait_send()


def on_device(fresh_keys, fresh_values, turn_angle):
    batch, length, _, size = fresh_keys.shape
    half_head = turn_angle.shape[1]
    pages = batch * length // PAGE
    vmem, any_space = pl.BlockSpec(memory_space=pltpu.VMEM), pl.BlockSpec(memory_space=pl.ANY)
    cache_keys, cache_values, high, low = pl.pallas_call(
        exchange,
        out_shape=(
            pltpu.VMEM((batch, length, size), jnp.bfloat16),
            pltpu.VMEM((batch, length, size), jnp.bfloat16),
            pltpu.VMEM((pages, size), jnp.bfloat16),
            pltpu.VMEM((pages, size), jnp.bfloat16),
        ),
        in_specs=[any_space] * 3,
        out_specs=(vmem,) * 4,
        scratch_shapes=[
            pltpu.VMEM((batch, length, size), jnp.bfloat16),
            pltpu.VMEM((batch, length, size), jnp.bfloat16),
            pltpu.VMEM((2, 2, 3, 3, length // 2, size), jnp.bfloat16),
            pltpu.VMEM((half_head, length), jnp.float32),
            pltpu.VMEM((length, size), jnp.float32),
            pltpu.VMEM((length, size), jnp.float32),
            pltpu.VMEM((pages, size), jnp.float32),
            pltpu.VMEM((pages, size), jnp.float32),
            pltpu.SemaphoreType.DMA((128,)),
            pltpu.SemaphoreType.DMA((128,)),
            pltpu.SemaphoreType.DMA((16,)),
            pltpu.SemaphoreType.DMA((2,)),
            pltpu.SemaphoreType.DMA,
        ],
        compiler_params=pltpu.CompilerParams(
            collective_id=0, has_side_effects=True, vmem_limit_bytes=40 * 2**20
        ),
    )(fresh_keys.reshape(batch, length, size), fresh_values.reshape(batch, length, size), turn_angle.T)
    return (
        cache_keys.reshape(1, -1, 1, size),
        cache_values.reshape(1, -1, 1, size),
        high.reshape(1, -1, 1, size),
        low.reshape(1, -1, 1, size),
    )


def solution(mesh):
    cut = P(None, ("coarse", "fine"), "model", None)
    whole = P(("coarse", "fine"), None, "model", None)
    return jax.shard_map(
        on_device, mesh=mesh, in_specs=(cut, cut, P()), out_specs=(whole,) * 4, check_vma=False
    )
```

```python
import jax
import jax.numpy as jnp
from jax import lax
from jax.experimental import pallas as pl
from jax.experimental.pallas import tpu as pltpu
from jax.sharding import PartitionSpec as P

PAGE = 32
SIDE = 4
MESH = pl.DeviceIdType.MESH
FAR_FIRST = (2, 1, 3)


def exchange(keys, values, angles, key_out, value_out, high_out, low_out, raw, turned, relay, angle, cosine, sine,
             tops, bottoms, send_sem, recv_sem, raw_sem, own_sem, angle_sem):
    length = keys.shape[1]
    half = length // 2
    coarse, fine, model = (lax.axis_index(name) for name in ("coarse", "fine", "model"))
    z, y = coarse * 2 + fine // SIDE, fine % SIDE
    me = z * SIDE + y

    def place(dz, dy):
        return (z + dz) % SIDE * SIDE + (y + dy) % SIDE

    def device(dz, dy):
        pz, py = (z + dz) % SIDE, (y + dy) % SIDE
        return (pz // 2, pz % 2 * SIDE + py, model)

    sources = (values, turned)
    outs = (value_out, key_out)

    def ring(way, step):
        return (0, step) if way == 0 else (step, 0)

    def both(way, first, second):
        return (second, first) if way == 0 else (first, second)

    def hop(item, way, leg, first, second):
        rows = pl.ds(way * half, half)
        at = place(*both(way, first, second))
        if leg == 0:
            src = sources[item].at[at, rows]
            if second == 0:
                dst = outs[item].at[me, rows]
            else:
                dst = relay.at[item, way, first - 1, second - 1]
            to = device(*ring(way, first))
        else:
            if first == 0:
                src = sources[item].at[at, rows]
                origin = me
            else:
                src = relay.at[item, way, first - 1, second - 1]
                origin = place(*both(way, -first, 0))
            dst = outs[item].at[origin, rows]
            to = device(*ring(1 - way, second))
        index = ((item * 2 + way) * 2 + leg) * 16 + first * 4 + second
        return pltpu.make_async_remote_copy(
            src_ref=src, dst_ref=dst, send_sem=send_sem.at[index], recv_sem=recv_sem.at[index],
            device_id=to, device_id_type=MESH,
        )

    barrier = pltpu.get_barrier_semaphore()
    for step in (1, 3, 2):
        for way in (0, 1):
            pl.semaphore_signal(barrier, inc=1, device_id=device(*ring(way, step)), device_id_type=MESH)

    columns = pl.ds(pl.multiple_of(me * length, 128), length)
    angle_copy = pltpu.make_async_copy(angles.at[:, columns], angle, angle_sem)
    angle_copy.start()
    raw_copy = [pltpu.make_async_copy(keys.at[b], raw.at[b], raw_sem.at[b]) for b in range(16)]
    for copy in raw_copy:
        copy.start()
    pl.semaphore_wait(barrier, 6)

    started = []

    def start(*which):
        copy = hop(*which)
        copy.start()
        started.append(copy)

    def leave(item):
        for second in (1, 2, 3, 0):
            for first in FAR_FIRST:
                for way in (0, 1):
                    start(item, way, 0, first, second)

    def forward(item):
        for first in (0, 2, 1, 3):
            for second in FAR_FIRST:
                for way in (0, 1):
                    if first:
                        hop(item, way, 0, first, second).wait_recv()
                    start(item, way, 1, first, second)

    leave(0)
    own_value = pltpu.make_async_copy(values.at[me], value_out.at[me], own_sem.at[0])
    own_value.start()

    angle_copy.wait()
    for at in range(0, length, 128):
        block = angle[:, at:at + 128]
        c, s = jnp.cos(block), jnp.sin(block)
        cosine[at:at + 128, :] = jnp.concatenate([c, c], axis=0).T
        sine[at:at + 128, :] = jnp.concatenate([-s, s], axis=0).T

    def turn(b, _):
        pltpu.make_async_copy(keys.at[b], raw.at[b], raw_sem.at[b]).wait()

        def tile(i, _):
            rows = pl.ds(pl.multiple_of(i * 128, 128), 128)
            x = raw[b, rows, :].astype(jnp.float32)
            turned[b, rows, :] = (x * cosine[rows, :] + pltpu.roll(x, 64, 1) * sine[rows, :]).astype(jnp.bfloat16)
            return 0

        return lax.fori_loop(0, length // 128, tile, 0)

    lax.fori_loop(0, 16, turn, 0)
    leave(1)
    own_key = pltpu.make_async_copy(turned.at[me], key_out.at[me], own_sem.at[1])
    own_key.start()
    forward(0)
    forward(1)

    pages = half // PAGE

    def bounds(origin, way):
        base = origin * (2 * pages) + way * pages

        def group(i, _):
            x = key_out[origin, pl.ds(pl.multiple_of(way * half + i * 8 * PAGE, 8 * PAGE), 8 * PAGE), :]
            x = x.astype(jnp.float32).reshape(8, PAGE, x.shape[-1])
            rows = pl.ds(pl.multiple_of(base + i * 8, 8), 8)
            tops[rows, :] = jnp.max(x, axis=1)
            bottoms[rows, :] = jnp.min(x, axis=1)
            return 0

        lax.fori_loop(0, pages // 8, group, 0)

    own_key.wait()
    for way in (0, 1):
        bounds(me, way)
    for first in FAR_FIRST:
        for way in (0, 1):
            hop(1, way, 0, first, 0).wait_recv()
            bounds(place(*both(way, -first, 0)), way)
    for first in (0, 2, 1, 3):
        for second in FAR_FIRST:
            for way in (0, 1):
                hop(1, way, 1, first, second).wait_recv()
                bounds(place(*both(way, -first, -second)), way)
    high_out[...] = tops[...].astype(jnp.bfloat16)
    low_out[...] = bottoms[...].astype(jnp.bfloat16)
    own_value.wait()
    for way in (0, 1):
        for first in FAR_FIRST:
            hop(0, way, 0, first, 0).wait_recv()
        for first in range(4):
            for second in FAR_FIRST:
                hop(0, way, 1, first, second).wait_recv()
    for copy in started:
        copy.wait_send()


def write_out(*refs):
    count = (len(refs) - 1) // 2
    sems, copies = refs[-1], []
    for i in range(count):
        src, dst = refs[i], refs[count + i]
        parts = 4 if len(src.shape) == 3 else 1
        size = src.shape[0] // parts
        for part in range(parts):
            at = pl.ds(part * size, size)
            copies.append(pltpu.make_async_copy(src.at[at], dst.at[at], sems.at[len(copies)]))
            copies[-1].start()
    for copy in copies:
        copy.wait()


def on_device(fresh_keys, fresh_values, turn_angle):
    batch, length, _, size = fresh_keys.shape
    half_head = turn_angle.shape[1]
    pages = batch * length // PAGE
    vmem, any_space = pl.BlockSpec(memory_space=pltpu.VMEM), pl.BlockSpec(memory_space=pl.ANY)
    cache_keys, cache_values, high, low = pl.pallas_call(
        exchange,
        out_shape=(
            pltpu.VMEM((batch, length, size), jnp.bfloat16),
            pltpu.VMEM((batch, length, size), jnp.bfloat16),
            pltpu.VMEM((pages, size), jnp.bfloat16),
            pltpu.VMEM((pages, size), jnp.bfloat16),
        ),
        in_specs=[any_space] * 3,
        out_specs=(vmem,) * 4,
        scratch_shapes=[
            pltpu.VMEM((batch, length, size), jnp.bfloat16),
            pltpu.VMEM((batch, length, size), jnp.bfloat16),
            pltpu.VMEM((2, 2, 3, 3, length // 2, size), jnp.bfloat16),
            pltpu.VMEM((half_head, length), jnp.float32),
            pltpu.VMEM((length, size), jnp.float32),
            pltpu.VMEM((length, size), jnp.float32),
            pltpu.VMEM((pages, size), jnp.float32),
            pltpu.VMEM((pages, size), jnp.float32),
            pltpu.SemaphoreType.DMA((128,)),
            pltpu.SemaphoreType.DMA((128,)),
            pltpu.SemaphoreType.DMA((16,)),
            pltpu.SemaphoreType.DMA((2,)),
            pltpu.SemaphoreType.DMA,
        ],
        compiler_params=pltpu.CompilerParams(
            collective_id=0, has_side_effects=True, vmem_limit_bytes=40 * 2**20
        ),
    )(fresh_keys.reshape(batch, length, size), fresh_values.reshape(batch, length, size), turn_angle.T)
    moved = (cache_keys, cache_values, high, low)
    cache_keys, cache_values, high, low = pl.pallas_call(
        write_out,
        out_shape=tuple(jax.ShapeDtypeStruct(x.shape, x.dtype) for x in moved),
        in_specs=[vmem] * 4,
        out_specs=(any_space,) * 4,
        scratch_shapes=[pltpu.SemaphoreType.DMA((10,))],
        compiler_params=pltpu.CompilerParams(vmem_limit_bytes=2**20),
    )(*moved)
    return (
        cache_keys.reshape(1, -1, 1, size),
        cache_values.reshape(1, -1, 1, size),
        high.reshape(1, -1, 1, size),
        low.reshape(1, -1, 1, size),
    )


def solution(mesh):
    cut = P(None, ("coarse", "fine"), "model", None)
    whole = P(("coarse", "fine"), None, "model", None)
    return jax.shard_map(
        on_device, mesh=mesh, in_specs=(cut, cut, P()), out_specs=(whole,) * 4, check_vma=False
    )
```

```python
import jax
import jax.numpy as jnp
from jax import lax
from jax.experimental import pallas as pl
from jax.experimental.pallas import tpu as pltpu
from jax.sharding import PartitionSpec as P

PAGE = 32
SIDE = 4
MESH = pl.DeviceIdType.MESH
FAR_FIRST = (2, 1, 3)


def exchange(keys, values, angles, key_out, value_out, high_out, low_out, raw, turned, relay, angle, cosine, sine,
             tops, bottoms, send_sem, recv_sem, raw_sem, own_sem, angle_sem, ready):
    length = keys.shape[1]
    half = length // 2
    coarse, fine, model = (lax.axis_index(name) for name in ("coarse", "fine", "model"))
    z, y = coarse * 2 + fine // SIDE, fine % SIDE
    me = z * SIDE + y

    def place(dz, dy):
        return (z + dz) % SIDE * SIDE + (y + dy) % SIDE

    def device(dz, dy, at=model):
        pz, py = (z + dz) % SIDE, (y + dy) % SIDE
        return (pz // 2, pz % 2 * SIDE + py, at)

    sources = (values, turned)
    outs = (value_out, key_out)

    def ring(way, step):
        return (0, step) if way == 0 else (step, 0)

    def both(way, first, second):
        return (second, first) if way == 0 else (first, second)

    def hop(item, way, leg, first, second):
        rows = pl.ds(way * half, half)
        at = place(*both(way, first, second))
        if leg == 0:
            src = sources[item].at[at, rows]
            if second == 0:
                dst = outs[item].at[me, rows]
            else:
                dst = relay.at[item, way, first - 1, second - 1]
            to = device(*ring(way, first))
        else:
            if first == 0:
                src = sources[item].at[at, rows]
                origin = me
            else:
                src = relay.at[item, way, first - 1, second - 1]
                origin = place(*both(way, -first, 0))
            dst = outs[item].at[origin, rows]
            to = device(*ring(1 - way, second))
        index = ((item * 2 + way) * 2 + leg) * 16 + first * 4 + second
        return pltpu.make_async_remote_copy(
            src_ref=src, dst_ref=dst, send_sem=send_sem.at[index], recv_sem=recv_sem.at[index],
            device_id=to, device_id_type=MESH,
        )

    core = model % 2
    partner = (coarse, fine, model + 1 - 2 * core)
    barrier = pltpu.get_barrier_semaphore()
    for step in (1, 3, 2):
        for way in (0, 1):
            gatherer = device(*ring(way, step), model - core + way)
            pl.semaphore_signal(barrier, inc=1, device_id=gatherer, device_id_type=MESH)
    pl.semaphore_signal(barrier, inc=1, device_id=partner, device_id_type=MESH)

    columns = pl.ds(pl.multiple_of(me * length, 128), length)
    angle_copy = pltpu.make_async_copy(angles.at[:, columns], angle, angle_sem)
    angle_copy.start()
    raw_copy = [pltpu.make_async_copy(keys.at[b], raw.at[b], raw_sem.at[b]) for b in range(16)]
    for copy in raw_copy:
        copy.start()
    pl.semaphore_wait(barrier, 7)
    pl.semaphore_signal(ready, inc=1, device_id=partner, device_id_type=MESH)

    started = []

    def start(*which):
        hop(*which).start()
        started.append(which)

    def leave(item, ways):
        for second in (1, 2, 3, 0):
            for first in FAR_FIRST:
                for way in ways:
                    start(item, way, 0, first, second)

    def forward(item):
        for first in (0, 2, 1, 3):
            for second in FAR_FIRST:
                for way in (0, 1):
                    if first:
                        hop(item, way, 0, first, second).wait_recv()
                    start(item, way, 1, first, second)

    for mine in (0, 1):

        @pl.when(core == mine)
        def _():
            leave(0, (mine,))
            pl.semaphore_wait(ready, 1)
            leave(0, (1 - mine,))

    own_value = pltpu.make_async_copy(values.at[me], value_out.at[me], own_sem.at[0])
    own_value.start()

    angle_copy.wait()
    for at in range(0, length, 128):
        block = angle[:, at:at + 128]
        c, s = jnp.cos(block), jnp.sin(block)
        cosine[at:at + 128, :] = jnp.concatenate([c, c], axis=0).T
        sine[at:at + 128, :] = jnp.concatenate([-s, s], axis=0).T

    def turn(b, _):
        pltpu.make_async_copy(keys.at[b], raw.at[b], raw_sem.at[b]).wait()

        def tile(i, _):
            rows = pl.ds(pl.multiple_of(i * 128, 128), 128)
            x = raw[b, rows, :].astype(jnp.float32)
            turned[b, rows, :] = (x * cosine[rows, :] + pltpu.roll(x, 64, 1) * sine[rows, :]).astype(jnp.bfloat16)
            return 0

        return lax.fori_loop(0, length // 128, tile, 0)

    lax.fori_loop(0, 16, turn, 0)
    leave(1, (0, 1))
    own_key = pltpu.make_async_copy(turned.at[me], key_out.at[me], own_sem.at[1])
    own_key.start()
    forward(1)
    forward(0)

    pages = half // PAGE

    def bounds(origin, way):
        base = origin * (2 * pages) + way * pages

        def group(i, _):
            x = key_out[origin, pl.ds(pl.multiple_of(way * half + i * 8 * PAGE, 8 * PAGE), 8 * PAGE), :]
            x = x.astype(jnp.float32).reshape(8, PAGE, x.shape[-1])
            rows = pl.ds(pl.multiple_of(base + i * 8, 8), 8)
            tops[rows, :] = jnp.max(x, axis=1)
            bottoms[rows, :] = jnp.min(x, axis=1)
            return 0

        lax.fori_loop(0, pages // 8, group, 0)

    own_key.wait()
    for way in (0, 1):
        bounds(me, way)
    for first in FAR_FIRST:
        for way in (0, 1):
            hop(1, way, 0, first, 0).wait_recv()
            bounds(place(*both(way, -first, 0)), way)
    for first in (0, 2, 1, 3):
        for second in FAR_FIRST:
            for way in (0, 1):
                hop(1, way, 1, first, second).wait_recv()
                bounds(place(*both(way, -first, -second)), way)
    high_out[...] = tops[...].astype(jnp.bfloat16)
    low_out[...] = bottoms[...].astype(jnp.bfloat16)
    own_value.wait()
    for way in (0, 1):
        for first in FAR_FIRST:
            hop(0, way, 0, first, 0).wait_recv()
        for first in range(4):
            for second in FAR_FIRST:
                hop(0, way, 1, first, second).wait_recv()
    for which in sorted(set(started)):
        hop(*which).wait_send()


def write_out(*refs):
    count = (len(refs) - 1) // 2
    sems, copies = refs[-1], []
    for i in range(count):
        src, dst = refs[i], refs[count + i]
        parts = 4 if len(src.shape) == 3 else 1
        size = src.shape[0] // parts
        for part in range(parts):
            at = pl.ds(part * size, size)
            copies.append(pltpu.make_async_copy(src.at[at], dst.at[at], sems.at[len(copies)]))
            copies[-1].start()
    for copy in copies:
        copy.wait()


def on_device(fresh_keys, fresh_values, turn_angle):
    batch, length, _, size = fresh_keys.shape
    half_head = turn_angle.shape[1]
    pages = batch * length // PAGE
    vmem, any_space = pl.BlockSpec(memory_space=pltpu.VMEM), pl.BlockSpec(memory_space=pl.ANY)
    cache_keys, cache_values, high, low = pl.pallas_call(
        exchange,
        out_shape=(
            pltpu.VMEM((batch, length, size), jnp.bfloat16),
            pltpu.VMEM((batch, length, size), jnp.bfloat16),
            pltpu.VMEM((pages, size), jnp.bfloat16),
            pltpu.VMEM((pages, size), jnp.bfloat16),
        ),
        in_specs=[any_space] * 3,
        out_specs=(vmem,) * 4,
        scratch_shapes=[
            pltpu.VMEM((batch, length, size), jnp.bfloat16),
            pltpu.VMEM((batch, length, size), jnp.bfloat16),
            pltpu.VMEM((2, 2, 3, 3, length // 2, size), jnp.bfloat16),
            pltpu.VMEM((half_head, length), jnp.float32),
            pltpu.VMEM((length, size), jnp.float32),
            pltpu.VMEM((length, size), jnp.float32),
            pltpu.VMEM((pages, size), jnp.float32),
            pltpu.VMEM((pages, size), jnp.float32),
            pltpu.SemaphoreType.DMA((128,)),
            pltpu.SemaphoreType.DMA((128,)),
            pltpu.SemaphoreType.DMA((16,)),
            pltpu.SemaphoreType.DMA((2,)),
            pltpu.SemaphoreType.DMA,
            pltpu.SemaphoreType.REGULAR,
        ],
        compiler_params=pltpu.CompilerParams(
            collective_id=0, has_side_effects=True, vmem_limit_bytes=40 * 2**20
        ),
    )(fresh_keys.reshape(batch, length, size), fresh_values.reshape(batch, length, size), turn_angle.T)
    moved = (cache_keys, cache_values, high, low)
    cache_keys, cache_values, high, low = pl.pallas_call(
        write_out,
        out_shape=tuple(jax.ShapeDtypeStruct(x.shape, x.dtype) for x in moved),
        in_specs=[vmem] * 4,
        out_specs=(any_space,) * 4,
        scratch_shapes=[pltpu.SemaphoreType.DMA((10,))],
        compiler_params=pltpu.CompilerParams(vmem_limit_bytes=2**20),
    )(*moved)
    return (
        cache_keys.reshape(1, -1, 1, size),
        cache_values.reshape(1, -1, 1, size),
        high.reshape(1, -1, 1, size),
        low.reshape(1, -1, 1, size),
    )


def solution(mesh):
    cut = P(None, ("coarse", "fine"), "model", None)
    whole = P(("coarse", "fine"), None, "model", None)
    return jax.shard_map(
        on_device, mesh=mesh, in_specs=(cut, cut, P()), out_specs=(whole,) * 4, check_vma=False
    )
```

```python
import types

import jax
import jax.numpy as jnp
from jax import lax
from jax.experimental import pallas as pl
from jax.experimental.pallas import tpu as pltpu
from jax.sharding import PartitionSpec as P

PAGE = 32
SIDE = 4
MESH = pl.DeviceIdType.MESH
FAR_FIRST = (2, 1, 3)
GROUPS = (0, 2, 1, 3)
LATE = ((0, 1, 2, 3), ())


def layout(length):
    half = length // 2
    coarse, fine, model = (lax.axis_index(name) for name in ("coarse", "fine", "model"))
    z, y = coarse * 2 + fine // SIDE, fine % SIDE

    def place(dz, dy):
        return (z + dz) % SIDE * SIDE + (y + dy) % SIDE

    def device(dz, dy, at=model):
        pz, py = (z + dz) % SIDE, (y + dy) % SIDE
        return (pz // 2, pz % 2 * SIDE + py, at)

    def ring(way, step):
        return (0, step) if way == 0 else (step, 0)

    def both(way, first, second):
        return (second, first) if way == 0 else (first, second)

    def rows(way):
        return pl.ds(way * half, half)

    core = model % 2

    def on_late(first, late, body):
        cores = [c for c in (0, 1) if (first in LATE[c]) == late]
        if len(cores) == 2:
            body()
        elif cores:
            pl.when(core == cores[0])(body)

    return types.SimpleNamespace(
        half=half, coarse=coarse, model=model, fine=fine, me=z * SIDE + y, core=core, place=place, device=device,
        ring=ring, both=both, rows=rows, on_late=on_late,
    )


def page_bounds(keys, origin, way, tops, bottoms):
    half = keys.shape[1] // 2
    pages = half // PAGE
    base = origin * (2 * pages) + way * pages

    def group(i, _):
        x = keys[origin, pl.ds(pl.multiple_of(way * half + i * 8 * PAGE, 8 * PAGE), 8 * PAGE), :]
        x = x.astype(jnp.float32).reshape(8, PAGE, x.shape[-1])
        rows = pl.ds(pl.multiple_of(base + i * 8, 8), 8)
        tops[rows, :] = jnp.max(x, axis=1)
        bottoms[rows, :] = jnp.min(x, axis=1)
        return 0

    lax.fori_loop(0, pages // 8, group, 0)


def exchange(keys, values, angles, key_out, value_out, key_relay, tops, bottoms, raw, turned, value_relay, angle,
             cosine, sine, send_sem, recv_sem, raw_sem, own_sem, angle_sem, keep_sem, ready):
    length = keys.shape[1]
    at = layout(length)
    me, core, place, device, ring, both = at.me, at.core, at.place, at.device, at.ring, at.both
    sources = (values, turned)
    outs = (value_out, key_out)
    relays = (value_relay, key_relay)

    def hop(item, way, leg, first, second):
        rows = at.rows(way)
        goal = place(*both(way, first, second))
        if leg == 0:
            src = sources[item].at[goal, rows]
            if second == 0:
                dst = outs[item].at[me, rows]
            else:
                dst = relays[item].at[way, first, second - 1]
            to = device(*ring(way, first))
        else:
            if first == 0:
                src = sources[item].at[goal, rows]
                origin = me
            else:
                src = relays[item].at[way, first, second - 1]
                origin = place(*both(way, -first, 0))
            dst = outs[item].at[origin, rows]
            to = device(*ring(1 - way, second))
        index = ((item * 2 + way) * 2 + leg) * 16 + first * 4 + second
        return pltpu.make_async_remote_copy(
            src_ref=src, dst_ref=dst, send_sem=send_sem.at[index], recv_sem=recv_sem.at[index],
            device_id=to, device_id_type=MESH,
        )

    partner = (at.coarse, at.fine, at.model + 1 - 2 * core)
    barrier = pltpu.get_barrier_semaphore()
    for step in (1, 3, 2):
        for way in (0, 1):
            gatherer = device(*ring(way, step), at.model - core + way)
            pl.semaphore_signal(barrier, inc=1, device_id=gatherer, device_id_type=MESH)
    pl.semaphore_signal(barrier, inc=1, device_id=partner, device_id_type=MESH)

    columns = pl.ds(pl.multiple_of(me * length, 128), length)
    angle_copy = pltpu.make_async_copy(angles.at[:, columns], angle, angle_sem)
    angle_copy.start()
    for b in range(16):
        pltpu.make_async_copy(keys.at[b], raw.at[b], raw_sem.at[b]).start()
    pl.semaphore_wait(barrier, 7)
    pl.semaphore_signal(ready, inc=1, device_id=partner, device_id_type=MESH)

    def leave(item, ways):
        for second in (1, 2, 3, 0):
            for first in FAR_FIRST:
                for way in ways:
                    hop(item, way, 0, first, second).start()

    def forward(item, first):
        for second in FAR_FIRST:
            for way in (0, 1):
                if first:
                    hop(item, way, 0, first, second).wait_recv()
                hop(item, way, 1, first, second).start()

    for mine in (0, 1):

        @pl.when(core == mine)
        def _():
            leave(0, (mine,))
            pl.semaphore_wait(ready, 1)
            leave(0, (1 - mine,))

    own_value = pltpu.make_async_copy(values.at[me], value_out.at[me], own_sem.at[0])
    own_value.start()

    angle_copy.wait()
    for start in range(0, length, 128):
        block = angle[:, start:start + 128]
        c, s = jnp.cos(block), jnp.sin(block)
        cosine[start:start + 128, :] = jnp.concatenate([c, c], axis=0).T
        sine[start:start + 128, :] = jnp.concatenate([-s, s], axis=0).T

    def turn(b, _):
        pltpu.make_async_copy(keys.at[b], raw.at[b], raw_sem.at[b]).wait()

        def tile(i, _):
            rows = pl.ds(pl.multiple_of(i * 128, 128), 128)
            x = raw[b, rows, :].astype(jnp.float32)
            turned[b, rows, :] = (x * cosine[rows, :] + pltpu.roll(x, 64, 1) * sine[rows, :]).astype(jnp.bfloat16)
            return 0

        return lax.fori_loop(0, length // 128, tile, 0)

    lax.fori_loop(0, 16, turn, 0)
    leave(1, (0, 1))
    own_key = pltpu.make_async_copy(turned.at[me], key_out.at[me], own_sem.at[1])
    own_key.start()
    for first in GROUPS:
        at.on_late(first, False, lambda: forward(1, first))
    for first in GROUPS:
        forward(0, first)

    def keep(way, second):
        index = way * 3 + second - 1
        return pltpu.make_async_copy(
            turned.at[place(*both(way, 0, second)), at.rows(way)], key_relay.at[way, 0, second - 1], keep_sem.at[index]
        )

    def relayed(first):
        for second in FAR_FIRST:
            for way in (0, 1):
                if first:
                    hop(1, way, 0, first, second).wait_recv()
                else:
                    keep(way, second).wait()

    for way in (0, 1):
        for second in FAR_FIRST:
            at.on_late(0, True, lambda: keep(way, second).start())

    own_key.wait()
    for way in (0, 1):
        page_bounds(key_out, me, way, tops, bottoms)
    for first in FAR_FIRST:
        for way in (0, 1):
            hop(1, way, 0, first, 0).wait_recv()
            page_bounds(key_out, place(*both(way, -first, 0)), way, tops, bottoms)

    def arrive(first):
        for second in FAR_FIRST:
            for way in (0, 1):
                hop(1, way, 1, first, second).wait_recv()
                page_bounds(key_out, place(*both(way, -first, -second)), way, tops, bottoms)

    for first in GROUPS:
        at.on_late(first, False, lambda: arrive(first))
        at.on_late(first, True, lambda: relayed(first))
    own_value.wait()

    def left(item, first):
        for second in FAR_FIRST:
            for way in (0, 1):
                hop(item, way, 1, first, second).wait_send()

    for way in (0, 1):
        for first in FAR_FIRST:
            hop(0, way, 0, first, 0).wait_recv()
            for second in range(4):
                hop(0, way, 0, first, second).wait_send()
                hop(1, way, 0, first, second).wait_send()
        for first in range(4):
            for second in FAR_FIRST:
                hop(0, way, 1, first, second).wait_recv()
    for first in range(4):
        left(0, first)
        at.on_late(first, False, lambda: left(1, first))


def last_groups(relay, early_tops, early_bottoms, _, key_out, high_out, low_out, tops, bottoms, send_sem, recv_sem):
    at = layout(key_out.shape[1])
    place, both = at.place, at.both

    def hop(way, first, second):
        index = (way * 4 + first) * 4 + second
        return pltpu.make_async_remote_copy(
            src_ref=relay.at[way, first, second - 1],
            dst_ref=key_out.at[place(*both(way, -first, 0)), at.rows(way)],
            send_sem=send_sem.at[index], recv_sem=recv_sem.at[index],
            device_id=at.device(*at.ring(1 - way, second)), device_id_type=MESH,
        )

    barrier = pltpu.get_barrier_semaphore()
    for step in (1, 3, 2):
        for way in (0, 1):
            pl.semaphore_signal(barrier, inc=1, device_id=at.device(*at.ring(way, step)), device_id_type=MESH)
    pl.semaphore_wait(barrier, 6)

    def start(first):
        for second in FAR_FIRST:
            for way in (0, 1):
                hop(way, first, second).start()

    def arrive(first):
        for second in FAR_FIRST:
            for way in (0, 1):
                hop(way, first, second).wait_recv()
                page_bounds(key_out, place(*both(way, -first, -second)), way, tops, bottoms)

    def left(first):
        for second in FAR_FIRST:
            for way in (0, 1):
                hop(way, first, second).wait_send()

    for first in GROUPS:
        at.on_late(first, True, lambda: start(first))
    tops[...] = early_tops[...]
    bottoms[...] = early_bottoms[...]
    for first in GROUPS:
        at.on_late(first, True, lambda: arrive(first))
    high_out[...] = tops[...].astype(jnp.bfloat16)
    low_out[...] = bottoms[...].astype(jnp.bfloat16)
    for first in GROUPS:
        at.on_late(first, True, lambda: left(first))


def write_early(key_in, value_in, key_out, value_out, done, sems):
    at = layout(key_in.shape[1])

    def value_part(part):
        rows = pl.ds(part * 4, 4)
        return pltpu.make_async_copy(value_in.at[rows], value_out.at[rows], sems.at[part])

    def key_part(way, first, second):
        here = (at.place(*at.both(way, -first, -second)), at.rows(way))
        return pltpu.make_async_copy(key_in.at[here], key_out.at[here], sems.at[4 + (way * 4 + first) * 4 + second])

    def steps(first):
        return FAR_FIRST + (0,)

    def start(first):
        for second in steps(first):
            for way in (0, 1):
                key_part(way, first, second).start()

    def wait(first):
        for second in steps(first):
            for way in (0, 1):
                key_part(way, first, second).wait()

    def direct(first, act):
        for way in (0, 1):
            act(key_part(way, first, 0))

    done[...] = jnp.zeros_like(done)
    for part in range(4):
        value_part(part).start()
    for first in GROUPS:
        at.on_late(first, True, lambda: direct(first, lambda copy: copy.start()))
        at.on_late(first, False, lambda: start(first))
    for part in range(4):
        value_part(part).wait()
    for first in GROUPS:
        at.on_late(first, True, lambda: direct(first, lambda copy: copy.wait()))
        at.on_late(first, False, lambda: wait(first))


def write_late(_, key_in, high_in, low_in, key_out, high_out, low_out, sems):
    at = layout(key_in.shape[1])

    def key_part(way, first, second):
        here = (at.place(*at.both(way, -first, -second)), at.rows(way))
        return pltpu.make_async_copy(key_in.at[here], key_out.at[here], sems.at[(way * 4 + first) * 4 + second])

    def start(first):
        for second in FAR_FIRST:
            for way in (0, 1):
                key_part(way, first, second).start()

    def wait(first):
        for second in FAR_FIRST:
            for way in (0, 1):
                key_part(way, first, second).wait()

    high = pltpu.make_async_copy(high_in, high_out, sems.at[0])
    low = pltpu.make_async_copy(low_in, low_out, sems.at[16])
    high.start()
    low.start()
    for first in GROUPS:
        at.on_late(first, True, lambda: start(first))
    high.wait()
    low.wait()
    for first in GROUPS:
        at.on_late(first, True, lambda: wait(first))


def on_device(fresh_keys, fresh_values, turn_angle):
    batch, length, _, size = fresh_keys.shape
    half_head = turn_angle.shape[1]
    pages = batch * length // PAGE
    vmem, any_space = pl.BlockSpec(memory_space=pltpu.VMEM), pl.BlockSpec(memory_space=pl.ANY)
    whole, relay = (batch, length, size), (2, SIDE, SIDE - 1, length // 2, size)
    early_keys, early_values, key_relay, tops, bottoms = pl.pallas_call(
        exchange,
        out_shape=(
            pltpu.VMEM(whole, jnp.bfloat16),
            pltpu.VMEM(whole, jnp.bfloat16),
            pltpu.VMEM(relay, jnp.bfloat16),
            pltpu.VMEM((pages, size), jnp.float32),
            pltpu.VMEM((pages, size), jnp.float32),
        ),
        in_specs=[any_space] * 3,
        out_specs=(vmem,) * 5,
        scratch_shapes=[
            pltpu.VMEM(whole, jnp.bfloat16),
            pltpu.VMEM(whole, jnp.bfloat16),
            pltpu.VMEM(relay, jnp.bfloat16),
            pltpu.VMEM((half_head, length), jnp.float32),
            pltpu.VMEM((length, size), jnp.float32),
            pltpu.VMEM((length, size), jnp.float32),
            pltpu.SemaphoreType.DMA((128,)),
            pltpu.SemaphoreType.DMA((128,)),
            pltpu.SemaphoreType.DMA((16,)),
            pltpu.SemaphoreType.DMA((2,)),
            pltpu.SemaphoreType.DMA,
            pltpu.SemaphoreType.DMA((6,)),
            pltpu.SemaphoreType.REGULAR,
        ],
        compiler_params=pltpu.CompilerParams(
            collective_id=0, has_side_effects=True, vmem_limit_bytes=43 * 2**20
        ),
    )(fresh_keys.reshape(whole), fresh_values.reshape(whole), turn_angle.T)
    some_keys, cache_values, written = pl.pallas_call(
        write_early,
        out_shape=(jax.ShapeDtypeStruct(whole, jnp.bfloat16),) * 2 + (pltpu.VMEM((8, size), jnp.float32),),
        in_specs=[vmem] * 2,
        out_specs=(any_space, any_space, vmem),
        scratch_shapes=[pltpu.SemaphoreType.DMA((36,))],
        compiler_params=pltpu.CompilerParams(vmem_limit_bytes=2**20),
    )(early_keys, early_values)
    late_keys, high, low = pl.pallas_call(
        last_groups,
        out_shape=(
            pltpu.VMEM(whole, jnp.bfloat16),
            pltpu.VMEM((pages, size), jnp.bfloat16),
            pltpu.VMEM((pages, size), jnp.bfloat16),
        ),
        in_specs=[vmem] * 4,
        out_specs=(vmem,) * 3,
        scratch_shapes=[
            pltpu.VMEM((pages, size), jnp.float32),
            pltpu.VMEM((pages, size), jnp.float32),
            pltpu.SemaphoreType.DMA((32,)),
            pltpu.SemaphoreType.DMA((32,)),
        ],
        compiler_params=pltpu.CompilerParams(
            collective_id=1, has_side_effects=True, vmem_limit_bytes=4 * 2**20
        ),
    )(key_relay, tops, bottoms, written)
    cache_keys, high, low = pl.pallas_call(
        write_late,
        out_shape=(
            jax.ShapeDtypeStruct(whole, jnp.bfloat16),
            jax.ShapeDtypeStruct((pages, size), jnp.bfloat16),
            jax.ShapeDtypeStruct((pages, size), jnp.bfloat16),
        ),
        in_specs=[any_space] + [vmem] * 3,
        out_specs=(any_space,) * 3,
        input_output_aliases={0: 0},
        scratch_shapes=[pltpu.SemaphoreType.DMA((32,))],
        compiler_params=pltpu.CompilerParams(vmem_limit_bytes=2**20),
    )(some_keys, late_keys, high, low)
    return (
        cache_keys.reshape(1, -1, 1, size),
        cache_values.reshape(1, -1, 1, size),
        high.reshape(1, -1, 1, size),
        low.reshape(1, -1, 1, size),
    )


def solution(mesh):
    cut = P(None, ("coarse", "fine"), "model", None)
    whole = P(("coarse", "fine"), None, "model", None)
    return jax.shard_map(
        on_device, mesh=mesh, in_specs=(cut, cut, P()), out_specs=(whole,) * 4, check_vma=False
    )
```

```python
import types

import jax
import jax.numpy as jnp
from jax import lax
from jax.experimental import pallas as pl
from jax.experimental.pallas import tpu as pltpu
from jax.sharding import PartitionSpec as P

PAGE = 32
SIDE = 4
MESH = pl.DeviceIdType.MESH
FAR_FIRST = (2, 1, 3)
GROUPS = (0, 2, 1, 3)
LATE = (1, 2, 3)


def layout(length):
    half = length // 2
    coarse, fine, model = (lax.axis_index(name) for name in ("coarse", "fine", "model"))
    z, y = coarse * 2 + fine // SIDE, fine % SIDE

    def place(dz, dy):
        return (z + dz) % SIDE * SIDE + (y + dy) % SIDE

    def device(dz, dy, at=model):
        pz, py = (z + dz) % SIDE, (y + dy) % SIDE
        return (pz // 2, pz % 2 * SIDE + py, at)

    def ring(way, step):
        return (0, step) if way == 0 else (step, 0)

    def both(way, first, second):
        return (second, first) if way == 0 else (first, second)

    def rows(way):
        return pl.ds(way * half, half)

    core = model % 2

    def on_late(first, late, body):
        if first not in LATE:
            if not late:
                body()
        else:
            pl.when(core == (0 if late else 1))(body)

    return types.SimpleNamespace(
        half=half, coarse=coarse, model=model, fine=fine, me=z * SIDE + y, core=core, place=place, device=device,
        ring=ring, both=both, rows=rows, on_late=on_late,
    )


def page_bounds(keys, origin, way, tops, bottoms):
    half = keys.shape[1] // 2
    pages = half // PAGE
    base = origin * (2 * pages) + way * pages

    def group(i, _):
        x = keys[origin, pl.ds(pl.multiple_of(way * half + i * 8 * PAGE, 8 * PAGE), 8 * PAGE), :]
        x = x.astype(jnp.float32).reshape(8, PAGE, x.shape[-1])
        rows = pl.ds(pl.multiple_of(base + i * 8, 8), 8)
        tops[rows, :] = jnp.max(x, axis=1)
        bottoms[rows, :] = jnp.min(x, axis=1)
        return 0

    lax.fori_loop(0, pages // 8, group, 0)


def exchange(keys, values, angles, key_out, value_out, value_relay, high_out, low_out, raw, turned, key_relay, tops,
             bottoms, angle, cosine, sine, send_sem, recv_sem, raw_sem, own_sem, angle_sem, keep_sem, ready):
    length = keys.shape[1]
    at = layout(length)
    me, core, place, device, ring, both = at.me, at.core, at.place, at.device, at.ring, at.both
    sources = (values, turned)
    outs = (value_out, key_out)

    def held(item, way, first, second):
        if item:
            return key_relay.at[way, first - 1, second - 1]
        return value_relay.at[way, first, second - 1]

    def hop(item, way, leg, first, second):
        rows = at.rows(way)
        goal = place(*both(way, first, second))
        if leg == 0:
            src = sources[item].at[goal, rows]
            if second == 0:
                dst = outs[item].at[me, rows]
            else:
                dst = held(item, way, first, second)
            to = device(*ring(way, first))
        else:
            if first == 0:
                src = sources[item].at[goal, rows]
                origin = me
            else:
                src = held(item, way, first, second)
                origin = place(*both(way, -first, 0))
            dst = outs[item].at[origin, rows]
            to = device(*ring(1 - way, second))
        index = ((item * 2 + way) * 2 + leg) * 16 + first * 4 + second
        return pltpu.make_async_remote_copy(
            src_ref=src, dst_ref=dst, send_sem=send_sem.at[index], recv_sem=recv_sem.at[index],
            device_id=to, device_id_type=MESH,
        )

    partner = (at.coarse, at.fine, at.model + 1 - 2 * core)
    barrier = pltpu.get_barrier_semaphore()
    for step in (1, 3, 2):
        for way in (0, 1):
            gatherer = device(*ring(way, step), at.model - core + way)
            pl.semaphore_signal(barrier, inc=1, device_id=gatherer, device_id_type=MESH)
    pl.semaphore_signal(barrier, inc=1, device_id=partner, device_id_type=MESH)

    columns = pl.ds(pl.multiple_of(me * length, 128), length)
    angle_copy = pltpu.make_async_copy(angles.at[:, columns], angle, angle_sem)
    angle_copy.start()
    for b in range(16):
        pltpu.make_async_copy(keys.at[b], raw.at[b], raw_sem.at[b]).start()
    pl.semaphore_wait(barrier, 7)
    pl.semaphore_signal(ready, inc=1, device_id=partner, device_id_type=MESH)

    def leave(item, ways):
        for second in (1, 2, 3, 0):
            for first in FAR_FIRST:
                for way in ways:
                    hop(item, way, 0, first, second).start()

    def forward(item, first):
        for second in FAR_FIRST:
            for way in (0, 1):
                if first:
                    hop(item, way, 0, first, second).wait_recv()
                hop(item, way, 1, first, second).start()

    def sent(item, leg):
        for way in (0, 1):
            for first in range(1 - leg, 4):
                for second in FAR_FIRST if leg else range(4):
                    hop(item, way, leg, first, second).wait_send()

    def hold(item, leg):
        pl.when(core == 1)(lambda: sent(item, leg))

    for mine in (0, 1):

        @pl.when(core == mine)
        def _():
            leave(0, (mine,))
            pl.semaphore_wait(ready, 1)
            leave(0, (1 - mine,))

    own_value = pltpu.make_async_copy(values.at[me], value_out.at[me], own_sem.at[0])
    own_value.start()

    angle_copy.wait()
    for start in range(0, length, 128):
        block = angle[:, start:start + 128]
        c, s = jnp.cos(block), jnp.sin(block)
        cosine[start:start + 128, :] = jnp.concatenate([c, c], axis=0).T
        sine[start:start + 128, :] = jnp.concatenate([-s, s], axis=0).T

    def turn(b, _):
        pltpu.make_async_copy(keys.at[b], raw.at[b], raw_sem.at[b]).wait()

        def tile(i, _):
            rows = pl.ds(pl.multiple_of(i * 128, 128), 128)
            x = raw[b, rows, :].astype(jnp.float32)
            turned[b, rows, :] = (x * cosine[rows, :] + pltpu.roll(x, 64, 1) * sine[rows, :]).astype(jnp.bfloat16)
            return 0

        return lax.fori_loop(0, length // 128, tile, 0)

    lax.fori_loop(0, 16, turn, 0)
    hold(0, 0)
    leave(1, (0, 1))
    own_key = pltpu.make_async_copy(turned.at[me], key_out.at[me], own_sem.at[1])
    own_key.start()
    for first in GROUPS:
        forward(1, first)
    for first in GROUPS:
        at.on_late(first, False, lambda: forward(0, first))

    def keep(way, second):
        return pltpu.make_async_copy(
            values.at[place(*both(way, 0, second)), at.rows(way)], value_relay.at[way, 0, second - 1],
            keep_sem.at[way * 3 + second - 1],
        )

    for way in (0, 1):
        for second in FAR_FIRST:
            at.on_late(0, True, lambda: keep(way, second).start())

    own_key.wait()
    for way in (0, 1):
        page_bounds(key_out, me, way, tops, bottoms)
    for first in FAR_FIRST:
        for way in (0, 1):
            hop(1, way, 0, first, 0).wait_recv()
            page_bounds(key_out, place(*both(way, -first, 0)), way, tops, bottoms)
    for first in GROUPS:
        for second in FAR_FIRST:
            for way in (0, 1):
                hop(1, way, 1, first, second).wait_recv()
                page_bounds(key_out, place(*both(way, -first, -second)), way, tops, bottoms)
    high_out[...] = tops[...].astype(jnp.bfloat16)
    low_out[...] = bottoms[...].astype(jnp.bfloat16)
    own_value.wait()

    def relayed(first):
        for second in FAR_FIRST:
            for way in (0, 1):
                if first:
                    hop(0, way, 0, first, second).wait_recv()
                else:
                    keep(way, second).wait()

    def arrive(first):
        for second in FAR_FIRST:
            for way in (0, 1):
                hop(0, way, 1, first, second).wait_recv()
                hop(0, way, 1, first, second).wait_send()

    for way in (0, 1):
        for first in FAR_FIRST:
            hop(0, way, 0, first, 0).wait_recv()
    pl.when(core == 0)(lambda: sent(0, 0))
    sent(1, 0)
    sent(1, 1)
    for first in GROUPS:
        at.on_late(first, True, lambda: relayed(first))
        at.on_late(first, False, lambda: arrive(first))


def last_groups(relay, _, value_out, send_sem, recv_sem):
    at = layout(value_out.shape[1])

    def hop(way, first, second):
        index = (way * 4 + first) * 4 + second
        return pltpu.make_async_remote_copy(
            src_ref=relay.at[way, first, second - 1],
            dst_ref=value_out.at[at.place(*at.both(way, -first, 0)), at.rows(way)],
            send_sem=send_sem.at[index], recv_sem=recv_sem.at[index],
            device_id=at.device(*at.ring(1 - way, second)), device_id_type=MESH,
        )

    @pl.when(at.core == 0)
    def _():
        barrier = pltpu.get_barrier_semaphore()
        for step in (1, 3, 2):
            for way in (0, 1):
                pl.semaphore_signal(barrier, inc=1, device_id=at.device(*at.ring(way, step)), device_id_type=MESH)
        pl.semaphore_wait(barrier, 6)
        groups = [(way, first, second) for first in LATE for second in FAR_FIRST for way in (0, 1)]
        for which in groups:
            hop(*which).start()
        for which in groups:
            hop(*which).wait()


def piece(at, src, dst, sems, way, first, second):
    here = (at.place(*at.both(way, -first, -second)), at.rows(way))
    return pltpu.make_async_copy(src.at[here], dst.at[here], sems.at[(way * 4 + first) * 4 + second])


def write_early(key_in, value_in, high_in, low_in, key_out, value_out, high_out, low_out, done, sems):
    at = layout(key_in.shape[1])
    done[...] = jnp.zeros_like(done)
    copies = [
        pltpu.make_async_copy(key_in.at[pl.ds(4 * part, 4)], key_out.at[pl.ds(4 * part, 4)], sems.at[32 + part])
        for part in range(4)
    ]
    copies.append(pltpu.make_async_copy(high_in, high_out, sems.at[36]))
    copies.append(pltpu.make_async_copy(low_in, low_out, sems.at[37]))
    for copy in copies:
        copy.start()

    def each(first, seconds, act):
        for second in seconds:
            for way in (0, 1):
                act(piece(at, value_in, value_out, sems, way, first, second))

    for act in (lambda copy: copy.start(), lambda copy: copy.wait()):
        for first in GROUPS:
            each(first, (0,), act)
            at.on_late(first, False, lambda: each(first, FAR_FIRST, act))
    for copy in copies:
        copy.wait()


def write_late(_, value_in, value_out, sems):
    at = layout(value_in.shape[1])

    def each(first, act):
        for second in FAR_FIRST:
            for way in (0, 1):
                act(piece(at, value_in, value_out, sems, way, first, second))

    for act in (lambda copy: copy.start(), lambda copy: copy.wait()):
        for first in GROUPS:
            at.on_late(first, True, lambda: each(first, act))


def on_device(fresh_keys, fresh_values, turn_angle):
    batch, length, _, size = fresh_keys.shape
    half_head = turn_angle.shape[1]
    pages = batch * length // PAGE
    vmem, any_space = pl.BlockSpec(memory_space=pltpu.VMEM), pl.BlockSpec(memory_space=pl.ANY)
    whole, bounds = (batch, length, size), (pages, size)
    relay = (SIDE - 1, length // 2, size)
    early_keys, early_values, value_relay, high, low = pl.pallas_call(
        exchange,
        out_shape=(
            pltpu.VMEM(whole, jnp.bfloat16),
            pltpu.VMEM(whole, jnp.bfloat16),
            pltpu.VMEM((2, SIDE) + relay, jnp.bfloat16),
            pltpu.VMEM(bounds, jnp.bfloat16),
            pltpu.VMEM(bounds, jnp.bfloat16),
        ),
        in_specs=[any_space] * 3,
        out_specs=(vmem,) * 5,
        scratch_shapes=[
            pltpu.VMEM(whole, jnp.bfloat16),
            pltpu.VMEM(whole, jnp.bfloat16),
            pltpu.VMEM((2, SIDE - 1) + relay, jnp.bfloat16),
            pltpu.VMEM(bounds, jnp.float32),
            pltpu.VMEM(bounds, jnp.float32),
            pltpu.VMEM((half_head, length), jnp.float32),
            pltpu.VMEM((length, size), jnp.float32),
            pltpu.VMEM((length, size), jnp.float32),
            pltpu.SemaphoreType.DMA((128,)),
            pltpu.SemaphoreType.DMA((128,)),
            pltpu.SemaphoreType.DMA((16,)),
            pltpu.SemaphoreType.DMA((2,)),
            pltpu.SemaphoreType.DMA,
            pltpu.SemaphoreType.DMA((6,)),
            pltpu.SemaphoreType.REGULAR,
        ],
        compiler_params=pltpu.CompilerParams(
            collective_id=0, has_side_effects=True, vmem_limit_bytes=43 * 2**20
        ),
    )(fresh_keys.reshape(whole), fresh_values.reshape(whole), turn_angle.T)
    cache_keys, some_values, high, low, written = pl.pallas_call(
        write_early,
        out_shape=(
            jax.ShapeDtypeStruct(whole, jnp.bfloat16),
            jax.ShapeDtypeStruct(whole, jnp.bfloat16),
            jax.ShapeDtypeStruct(bounds, jnp.bfloat16),
            jax.ShapeDtypeStruct(bounds, jnp.bfloat16),
            pltpu.VMEM((8, size), jnp.float32),
        ),
        in_specs=[vmem] * 4,
        out_specs=(any_space,) * 4 + (vmem,),
        scratch_shapes=[pltpu.SemaphoreType.DMA((38,))],
        compiler_params=pltpu.CompilerParams(vmem_limit_bytes=2**20),
    )(early_keys, early_values, high, low)
    late_values = pl.pallas_call(
        last_groups,
        out_shape=pltpu.VMEM(whole, jnp.bfloat16),
        in_specs=[vmem] * 2,
        out_specs=vmem,
        scratch_shapes=[pltpu.SemaphoreType.DMA((32,)), pltpu.SemaphoreType.DMA((32,))],
        compiler_params=pltpu.CompilerParams(
            collective_id=1, has_side_effects=True, vmem_limit_bytes=4 * 2**20
        ),
    )(value_relay, written)
    cache_values = pl.pallas_call(
        write_late,
        out_shape=jax.ShapeDtypeStruct(whole, jnp.bfloat16),
        in_specs=[any_space, vmem],
        out_specs=any_space,
        input_output_aliases={0: 0},
        scratch_shapes=[pltpu.SemaphoreType.DMA((32,))],
        compiler_params=pltpu.CompilerParams(vmem_limit_bytes=2**20),
    )(some_values, late_values)
    return (
        cache_keys.reshape(1, -1, 1, size),
        cache_values.reshape(1, -1, 1, size),
        high.reshape(1, -1, 1, size),
        low.reshape(1, -1, 1, size),
    )


def solution(mesh):
    cut = P(None, ("coarse", "fine"), "model", None)
    whole = P(("coarse", "fine"), None, "model", None)
    return jax.shard_map(
        on_device, mesh=mesh, in_specs=(cut, cut, P()), out_specs=(whole,) * 4, check_vma=False
    )
```

```python
import types

import jax
import jax.numpy as jnp
from jax import lax
from jax.experimental import pallas as pl
from jax.experimental.pallas import tpu as pltpu
from jax.sharding import PartitionSpec as P

PAGE = 32
SIDE = 4
MESH = pl.DeviceIdType.MESH
FAR_FIRST = (2, 1, 3)
GROUPS = (0, 2, 1, 3)
LATE = (1, 2, 3)


def layout(length):
    half = length // 2
    coarse, fine, model = (lax.axis_index(name) for name in ("coarse", "fine", "model"))
    z, y = coarse * 2 + fine // SIDE, fine % SIDE

    def place(dz, dy):
        return (z + dz) % SIDE * SIDE + (y + dy) % SIDE

    def device(dz, dy, at=model):
        pz, py = (z + dz) % SIDE, (y + dy) % SIDE
        return (pz // 2, pz % 2 * SIDE + py, at)

    def ring(way, step):
        return (0, step) if way == 0 else (step, 0)

    def both(way, first, second):
        return (second, first) if way == 0 else (first, second)

    def rows(way):
        return pl.ds(way * half, half)

    core = model % 2

    def on_late(first, late, body):
        if first not in LATE:
            if not late:
                body()
        else:
            pl.when(core == (0 if late else 1))(body)

    return types.SimpleNamespace(
        half=half, coarse=coarse, model=model, fine=fine, me=z * SIDE + y, core=core, place=place, device=device,
        ring=ring, both=both, rows=rows, on_late=on_late,
    )


def page_bounds(keys, origin, way, tops, bottoms):
    half = keys.shape[1] // 2
    pages = half // PAGE
    base = origin * (2 * pages) + way * pages

    def group(i, _):
        x = keys[origin, pl.ds(pl.multiple_of(way * half + i * 8 * PAGE, 8 * PAGE), 8 * PAGE), :]
        x = x.astype(jnp.float32).reshape(8, PAGE, x.shape[-1])
        rows = pl.ds(pl.multiple_of(base + i * 8, 8), 8)
        tops[rows, :] = jnp.max(x, axis=1)
        bottoms[rows, :] = jnp.min(x, axis=1)
        return 0

    lax.fori_loop(0, pages // 8, group, 0)


def exchange(keys, values, angles, key_out, value_out, value_relay, high_out, low_out, raw, turned, key_relay, tops,
             bottoms, angle, cosine, sine, send_sem, recv_sem, raw_sem, own_sem, angle_sem, keep_sem, ready):
    length = keys.shape[1]
    at = layout(length)
    me, core, place, device, ring, both = at.me, at.core, at.place, at.device, at.ring, at.both
    sources = (values, turned)
    outs = (value_out, key_out)

    def held(item, way, first, second):
        if item:
            return key_relay.at[way, first - 1, second - 1]
        return value_relay.at[way, first, second - 1]

    def hop(item, way, leg, first, second):
        rows = at.rows(way)
        goal = place(*both(way, first, second))
        if leg == 0:
            src = sources[item].at[goal, rows]
            if second == 0:
                dst = outs[item].at[me, rows]
            else:
                dst = held(item, way, first, second)
            to = device(*ring(way, first))
        else:
            if first == 0:
                src = sources[item].at[goal, rows]
                origin = me
            else:
                src = held(item, way, first, second)
                origin = place(*both(way, -first, 0))
            dst = outs[item].at[origin, rows]
            to = device(*ring(1 - way, second))
        index = ((item * 2 + way) * 2 + leg) * 16 + first * 4 + second
        return pltpu.make_async_remote_copy(
            src_ref=src, dst_ref=dst, send_sem=send_sem.at[index], recv_sem=recv_sem.at[index],
            device_id=to, device_id_type=MESH,
        )

    partner = (at.coarse, at.fine, at.model + 1 - 2 * core)
    barrier = pltpu.get_barrier_semaphore()
    for step in (1, 3, 2):
        for way in (0, 1):
            gatherer = device(*ring(way, step), at.model - core + way)
            pl.semaphore_signal(barrier, inc=1, device_id=gatherer, device_id_type=MESH)
    pl.semaphore_signal(barrier, inc=1, device_id=partner, device_id_type=MESH)

    columns = pl.ds(pl.multiple_of(me * length, 128), length)
    angle_copy = pltpu.make_async_copy(angles.at[:, columns], angle, angle_sem)
    angle_copy.start()
    for b in range(16):
        pltpu.make_async_copy(keys.at[b], raw.at[b], raw_sem.at[b]).start()
    pl.semaphore_wait(barrier, 7)
    pl.semaphore_signal(ready, inc=1, device_id=partner, device_id_type=MESH)

    def leave(item, ways):
        for second in (1, 2, 3, 0):
            for first in FAR_FIRST:
                for way in ways:
                    hop(item, way, 0, first, second).start()

    def forward(item, first):
        for second in FAR_FIRST:
            for way in (0, 1):
                if first:
                    hop(item, way, 0, first, second).wait_recv()
                hop(item, way, 1, first, second).start()

    def sent(item, leg):
        for way in (0, 1):
            for first in range(1 - leg, 4):
                for second in FAR_FIRST if leg else range(4):
                    hop(item, way, leg, first, second).wait_send()

    for mine in (0, 1):

        @pl.when(core == mine)
        def _():
            leave(0, (mine,))
            pl.semaphore_wait(ready, 1)
            leave(0, (1 - mine,))

    own_value = pltpu.make_async_copy(values.at[me], value_out.at[me], own_sem.at[0])
    own_value.start()

    angle_copy.wait()
    for start in range(0, length, 128):
        block = angle[:, start:start + 128]
        c, s = jnp.cos(block), jnp.sin(block)
        cosine[start:start + 128, :] = jnp.concatenate([c, c], axis=0).T
        sine[start:start + 128, :] = jnp.concatenate([-s, s], axis=0).T

    def turn(b, _):
        pltpu.make_async_copy(keys.at[b], raw.at[b], raw_sem.at[b]).wait()

        def tile(i, _):
            rows = pl.ds(pl.multiple_of(i * 128, 128), 128)
            x = raw[b, rows, :].astype(jnp.float32)
            turned[b, rows, :] = (x * cosine[rows, :] + pltpu.roll(x, 64, 1) * sine[rows, :]).astype(jnp.bfloat16)
            return 0

        return lax.fori_loop(0, length // 128, tile, 0)

    lax.fori_loop(0, 16, turn, 0)
    @pl.when(core == 0)
    def _():
        leave(1, (0, 1))

    @pl.when(core == 1)
    def _():
        sent(0, 0)
        for second in (1, 2, 3, 0):
            batch = [hop(1, way, 0, first, second) for first in FAR_FIRST for way in (0, 1)]
            for copy in batch:
                copy.start()
            for copy in batch:
                copy.wait_send()

    own_key = pltpu.make_async_copy(turned.at[me], key_out.at[me], own_sem.at[1])
    own_key.start()
    for first in GROUPS:
        forward(1, first)
    for first in GROUPS:
        at.on_late(first, False, lambda: forward(0, first))

    def keep(way, second):
        return pltpu.make_async_copy(
            values.at[place(*both(way, 0, second)), at.rows(way)], value_relay.at[way, 0, second - 1],
            keep_sem.at[way * 3 + second - 1],
        )

    for way in (0, 1):
        for second in FAR_FIRST:
            at.on_late(0, True, lambda: keep(way, second).start())

    own_key.wait()
    for way in (0, 1):
        page_bounds(key_out, me, way, tops, bottoms)
    for first in FAR_FIRST:
        for way in (0, 1):
            hop(1, way, 0, first, 0).wait_recv()
            page_bounds(key_out, place(*both(way, -first, 0)), way, tops, bottoms)
    for first in GROUPS:
        for second in FAR_FIRST:
            for way in (0, 1):
                hop(1, way, 1, first, second).wait_recv()
                page_bounds(key_out, place(*both(way, -first, -second)), way, tops, bottoms)
    high_out[...] = tops[...].astype(jnp.bfloat16)
    low_out[...] = bottoms[...].astype(jnp.bfloat16)
    own_value.wait()

    def relayed(first):
        for second in FAR_FIRST:
            for way in (0, 1):
                if first:
                    hop(0, way, 0, first, second).wait_recv()
                else:
                    keep(way, second).wait()

    def arrive(first):
        for second in FAR_FIRST:
            for way in (0, 1):
                hop(0, way, 1, first, second).wait_recv()
                hop(0, way, 1, first, second).wait_send()

    for way in (0, 1):
        for first in FAR_FIRST:
            hop(0, way, 0, first, 0).wait_recv()
    pl.when(core == 0)(lambda: sent(0, 0))
    pl.when(core == 0)(lambda: sent(1, 0))
    sent(1, 1)
    for first in GROUPS:
        at.on_late(first, True, lambda: relayed(first))
        at.on_late(first, False, lambda: arrive(first))


def last_groups(relay, _, value_out, send_sem, recv_sem):
    at = layout(value_out.shape[1])

    def hop(way, first, second):
        index = (way * 4 + first) * 4 + second
        return pltpu.make_async_remote_copy(
            src_ref=relay.at[way, first, second - 1],
            dst_ref=value_out.at[at.place(*at.both(way, -first, 0)), at.rows(way)],
            send_sem=send_sem.at[index], recv_sem=recv_sem.at[index],
            device_id=at.device(*at.ring(1 - way, second)), device_id_type=MESH,
        )

    @pl.when(at.core == 0)
    def _():
        barrier = pltpu.get_barrier_semaphore()
        for step in (1, 3, 2):
            for way in (0, 1):
                pl.semaphore_signal(barrier, inc=1, device_id=at.device(*at.ring(way, step)), device_id_type=MESH)
        pl.semaphore_wait(barrier, 6)
        groups = [(way, first, second) for first in LATE for second in FAR_FIRST for way in (0, 1)]
        for which in groups:
            hop(*which).start()
        for which in groups:
            hop(*which).wait()


def piece(at, src, dst, sems, way, first, second):
    here = (at.place(*at.both(way, -first, -second)), at.rows(way))
    return pltpu.make_async_copy(src.at[here], dst.at[here], sems.at[(way * 4 + first) * 4 + second])


def write_early(key_in, value_in, high_in, low_in, key_out, value_out, high_out, low_out, done, sems):
    at = layout(key_in.shape[1])
    done[...] = jnp.zeros_like(done)
    copies = [
        pltpu.make_async_copy(key_in.at[pl.ds(4 * part, 4)], key_out.at[pl.ds(4 * part, 4)], sems.at[32 + part])
        for part in range(4)
    ]
    copies.append(pltpu.make_async_copy(high_in, high_out, sems.at[36]))
    copies.append(pltpu.make_async_copy(low_in, low_out, sems.at[37]))
    for copy in copies:
        copy.start()

    def each(first, seconds, act):
        for second in seconds:
            for way in (0, 1):
                act(piece(at, value_in, value_out, sems, way, first, second))

    for act in (lambda copy: copy.start(), lambda copy: copy.wait()):
        for first in GROUPS:
            each(first, (0,), act)
            at.on_late(first, False, lambda: each(first, FAR_FIRST, act))
    for copy in copies:
        copy.wait()


def write_late(_, value_in, value_out, sems):
    at = layout(value_in.shape[1])

    def each(first, act):
        for second in FAR_FIRST:
            for way in (0, 1):
                act(piece(at, value_in, value_out, sems, way, first, second))

    for act in (lambda copy: copy.start(), lambda copy: copy.wait()):
        for first in GROUPS:
            at.on_late(first, True, lambda: each(first, act))


def on_device(fresh_keys, fresh_values, turn_angle):
    batch, length, _, size = fresh_keys.shape
    half_head = turn_angle.shape[1]
    pages = batch * length // PAGE
    vmem, any_space = pl.BlockSpec(memory_space=pltpu.VMEM), pl.BlockSpec(memory_space=pl.ANY)
    whole, bounds = (batch, length, size), (pages, size)
    relay = (SIDE - 1, length // 2, size)
    early_keys, early_values, value_relay, high, low = pl.pallas_call(
        exchange,
        out_shape=(
            pltpu.VMEM(whole, jnp.bfloat16),
            pltpu.VMEM(whole, jnp.bfloat16),
            pltpu.VMEM((2, SIDE) + relay, jnp.bfloat16),
            pltpu.VMEM(bounds, jnp.bfloat16),
            pltpu.VMEM(bounds, jnp.bfloat16),
        ),
        in_specs=[any_space] * 3,
        out_specs=(vmem,) * 5,
        scratch_shapes=[
            pltpu.VMEM(whole, jnp.bfloat16),
            pltpu.VMEM(whole, jnp.bfloat16),
            pltpu.VMEM((2, SIDE - 1) + relay, jnp.bfloat16),
            pltpu.VMEM(bounds, jnp.float32),
            pltpu.VMEM(bounds, jnp.float32),
            pltpu.VMEM((half_head, length), jnp.float32),
            pltpu.VMEM((length, size), jnp.float32),
            pltpu.VMEM((length, size), jnp.float32),
            pltpu.SemaphoreType.DMA((128,)),
            pltpu.SemaphoreType.DMA((128,)),
            pltpu.SemaphoreType.DMA((16,)),
            pltpu.SemaphoreType.DMA((2,)),
            pltpu.SemaphoreType.DMA,
            pltpu.SemaphoreType.DMA((6,)),
            pltpu.SemaphoreType.REGULAR,
        ],
        compiler_params=pltpu.CompilerParams(
            collective_id=0, has_side_effects=True, vmem_limit_bytes=43 * 2**20
        ),
    )(fresh_keys.reshape(whole), fresh_values.reshape(whole), turn_angle.T)
    cache_keys, some_values, high, low, written = pl.pallas_call(
        write_early,
        out_shape=(
            jax.ShapeDtypeStruct(whole, jnp.bfloat16),
            jax.ShapeDtypeStruct(whole, jnp.bfloat16),
            jax.ShapeDtypeStruct(bounds, jnp.bfloat16),
            jax.ShapeDtypeStruct(bounds, jnp.bfloat16),
            pltpu.VMEM((8, size), jnp.float32),
        ),
        in_specs=[vmem] * 4,
        out_specs=(any_space,) * 4 + (vmem,),
        scratch_shapes=[pltpu.SemaphoreType.DMA((38,))],
        compiler_params=pltpu.CompilerParams(vmem_limit_bytes=2**20),
    )(early_keys, early_values, high, low)
    late_values = pl.pallas_call(
        last_groups,
        out_shape=pltpu.VMEM(whole, jnp.bfloat16),
        in_specs=[vmem] * 2,
        out_specs=vmem,
        scratch_shapes=[pltpu.SemaphoreType.DMA((32,)), pltpu.SemaphoreType.DMA((32,))],
        compiler_params=pltpu.CompilerParams(
            collective_id=1, has_side_effects=True, vmem_limit_bytes=4 * 2**20
        ),
    )(value_relay, written)
    cache_values = pl.pallas_call(
        write_late,
        out_shape=jax.ShapeDtypeStruct(whole, jnp.bfloat16),
        in_specs=[any_space, vmem],
        out_specs=any_space,
        input_output_aliases={0: 0},
        scratch_shapes=[pltpu.SemaphoreType.DMA((32,))],
        compiler_params=pltpu.CompilerParams(vmem_limit_bytes=2**20),
    )(some_values, late_values)
    return (
        cache_keys.reshape(1, -1, 1, size),
        cache_values.reshape(1, -1, 1, size),
        high.reshape(1, -1, 1, size),
        low.reshape(1, -1, 1, size),
    )


def solution(mesh):
    cut = P(None, ("coarse", "fine"), "model", None)
    whole = P(("coarse", "fine"), None, "model", None)
    return jax.shard_map(
        on_device, mesh=mesh, in_specs=(cut, cut, P()), out_specs=(whole,) * 4, check_vma=False
    )
```

```python
import types

import jax
import jax.numpy as jnp
from jax import lax
from jax.experimental import pallas as pl
from jax.experimental.pallas import tpu as pltpu
from jax.sharding import PartitionSpec as P

PAGE = 32
SIDE = 4
MESH = pl.DeviceIdType.MESH
FAR_FIRST = (2, 1, 3)
GROUPS = (0, 2, 1, 3)
LATE = (1, 2, 3)


def layout(length):
    half = length // 2
    coarse, fine, model = (lax.axis_index(name) for name in ("coarse", "fine", "model"))
    z, y = coarse * 2 + fine // SIDE, fine % SIDE

    def place(dz, dy):
        return (z + dz) % SIDE * SIDE + (y + dy) % SIDE

    def device(dz, dy, at=model):
        pz, py = (z + dz) % SIDE, (y + dy) % SIDE
        return (pz // 2, pz % 2 * SIDE + py, at)

    def ring(way, step):
        return (0, step) if way == 0 else (step, 0)

    def both(way, first, second):
        return (second, first) if way == 0 else (first, second)

    def rows(way):
        return pl.ds(way * half, half)

    core = model % 2

    def on_late(first, late, body):
        if first not in LATE:
            if not late:
                body()
        else:
            pl.when(core == (0 if late else 1))(body)

    return types.SimpleNamespace(
        half=half, coarse=coarse, model=model, fine=fine, me=z * SIDE + y, core=core, place=place, device=device,
        ring=ring, both=both, rows=rows, on_late=on_late,
    )


def page_bounds(keys, origin, way, tops, bottoms):
    half = keys.shape[1] // 2
    pages = half // PAGE
    base = origin * (2 * pages) + way * pages

    def group(i, _):
        x = keys[origin, pl.ds(pl.multiple_of(way * half + i * 8 * PAGE, 8 * PAGE), 8 * PAGE), :]
        x = x.astype(jnp.float32).reshape(8, PAGE, x.shape[-1])
        rows = pl.ds(pl.multiple_of(base + i * 8, 8), 8)
        tops[rows, :] = jnp.max(x, axis=1)
        bottoms[rows, :] = jnp.min(x, axis=1)
        return 0

    lax.fori_loop(0, pages // 8, group, 0)


def exchange(keys, values, angles, key_out, value_out, value_relay, high_out, low_out, raw, turned, key_relay, tops,
             bottoms, angle, cosine, sine, send_sem, recv_sem, raw_sem, own_sem, angle_sem, keep_sem, ready):
    length = keys.shape[1]
    at = layout(length)
    me, core, place, device, ring, both = at.me, at.core, at.place, at.device, at.ring, at.both
    sources = (values, turned)
    outs = (value_out, key_out)

    def held(item, way, first, second):
        if item:
            return key_relay.at[way, first - 1, second - 1]
        return value_relay.at[way, first, second - 1]

    def hop(item, way, leg, first, second):
        rows = at.rows(way)
        goal = place(*both(way, first, second))
        if leg == 0:
            src = sources[item].at[goal, rows]
            if second == 0:
                dst = outs[item].at[me, rows]
            else:
                dst = held(item, way, first, second)
            to = device(*ring(way, first))
        else:
            if first == 0:
                src = sources[item].at[goal, rows]
                origin = me
            else:
                src = held(item, way, first, second)
                origin = place(*both(way, -first, 0))
            dst = outs[item].at[origin, rows]
            to = device(*ring(1 - way, second))
        index = ((item * 2 + way) * 2 + leg) * 16 + first * 4 + second
        return pltpu.make_async_remote_copy(
            src_ref=src, dst_ref=dst, send_sem=send_sem.at[index], recv_sem=recv_sem.at[index],
            device_id=to, device_id_type=MESH,
        )

    partner = (at.coarse, at.fine, at.model + 1 - 2 * core)
    barrier = pltpu.get_barrier_semaphore()
    for step in (1, 3, 2):
        for way in (0, 1):
            gatherer = device(*ring(way, step), at.model - core + way)
            pl.semaphore_signal(barrier, inc=1, device_id=gatherer, device_id_type=MESH)
    pl.semaphore_signal(barrier, inc=1, device_id=partner, device_id_type=MESH)

    columns = pl.ds(pl.multiple_of(me * length, 128), length)
    angle_copy = pltpu.make_async_copy(angles.at[:, columns], angle, angle_sem)
    angle_copy.start()
    for b in range(16):
        pltpu.make_async_copy(keys.at[b], raw.at[b], raw_sem.at[b]).start()
    pl.semaphore_wait(barrier, 7)
    pl.semaphore_signal(ready, inc=1, device_id=partner, device_id_type=MESH)

    def leave(item, ways):
        for second in (1, 2, 3, 0):
            for first in FAR_FIRST:
                for way in ways:
                    hop(item, way, 0, first, second).start()

    def forward(item, first):
        for second in FAR_FIRST:
            for way in (0, 1):
                if first:
                    hop(item, way, 0, first, second).wait_recv()
                hop(item, way, 1, first, second).start()

    def sent(item, leg):
        for way in (0, 1):
            for first in range(1 - leg, 4):
                for second in FAR_FIRST if leg else range(4):
                    hop(item, way, leg, first, second).wait_send()

    def hold(item, leg):
        pl.when(core == 1)(lambda: sent(item, leg))

    for mine in (0, 1):

        @pl.when(core == mine)
        def _():
            leave(0, (mine,))
            pl.semaphore_wait(ready, 1)
            leave(0, (1 - mine,))

    own_value = pltpu.make_async_copy(values.at[me], value_out.at[me], own_sem.at[0])
    own_value.start()

    angle_copy.wait()
    for start in range(0, length, 128):
        block = angle[:, start:start + 128]
        c, s = jnp.cos(block), jnp.sin(block)
        cosine[start:start + 128, :] = jnp.concatenate([c, c], axis=0).T
        sine[start:start + 128, :] = jnp.concatenate([-s, s], axis=0).T

    def turn(b, _):
        pltpu.make_async_copy(keys.at[b], raw.at[b], raw_sem.at[b]).wait()

        def tile(i, _):
            rows = pl.ds(pl.multiple_of(i * 128, 128), 128)
            x = raw[b, rows, :].astype(jnp.float32)
            turned[b, rows, :] = (x * cosine[rows, :] + pltpu.roll(x, 64, 1) * sine[rows, :]).astype(jnp.bfloat16)
            return 0

        return lax.fori_loop(0, length // 128, tile, 0)

    lax.fori_loop(0, 16, turn, 0)
    hold(0, 0)
    leave(1, (0, 1))
    own_key = pltpu.make_async_copy(turned.at[me], key_out.at[me], own_sem.at[1])
    own_key.start()
    hold(1, 0)
    for first in GROUPS:
        forward(1, first)
    for first in GROUPS:
        at.on_late(first, False, lambda: forward(0, first))

    def keep(way, second):
        return pltpu.make_async_copy(
            values.at[place(*both(way, 0, second)), at.rows(way)], value_relay.at[way, 0, second - 1],
            keep_sem.at[way * 3 + second - 1],
        )

    for way in (0, 1):
        for second in FAR_FIRST:
            at.on_late(0, True, lambda: keep(way, second).start())

    own_key.wait()
    for way in (0, 1):
        page_bounds(key_out, me, way, tops, bottoms)
    for first in FAR_FIRST:
        for way in (0, 1):
            hop(1, way, 0, first, 0).wait_recv()
            page_bounds(key_out, place(*both(way, -first, 0)), way, tops, bottoms)
    for first in GROUPS:
        for second in FAR_FIRST:
            for way in (0, 1):
                hop(1, way, 1, first, second).wait_recv()
                page_bounds(key_out, place(*both(way, -first, -second)), way, tops, bottoms)
    high_out[...] = tops[...].astype(jnp.bfloat16)
    low_out[...] = bottoms[...].astype(jnp.bfloat16)
    own_value.wait()

    def relayed(first):
        for second in FAR_FIRST:
            for way in (0, 1):
                if first:
                    hop(0, way, 0, first, second).wait_recv()
                else:
                    keep(way, second).wait()

    def arrive(first):
        for second in FAR_FIRST:
            for way in (0, 1):
                hop(0, way, 1, first, second).wait_recv()
                hop(0, way, 1, first, second).wait_send()

    for way in (0, 1):
        for first in FAR_FIRST:
            hop(0, way, 0, first, 0).wait_recv()
    pl.when(core == 0)(lambda: sent(0, 0))
    pl.when(core == 0)(lambda: sent(1, 0))
    sent(1, 1)
    for first in GROUPS:
        at.on_late(first, True, lambda: relayed(first))
        at.on_late(first, False, lambda: arrive(first))


def last_groups(relay, _, value_out, send_sem, recv_sem):
    at = layout(value_out.shape[1])

    def hop(way, first, second):
        index = (way * 4 + first) * 4 + second
        return pltpu.make_async_remote_copy(
            src_ref=relay.at[way, first, second - 1],
            dst_ref=value_out.at[at.place(*at.both(way, -first, 0)), at.rows(way)],
            send_sem=send_sem.at[index], recv_sem=recv_sem.at[index],
            device_id=at.device(*at.ring(1 - way, second)), device_id_type=MESH,
        )

    @pl.when(at.core == 0)
    def _():
        barrier = pltpu.get_barrier_semaphore()
        for step in (1, 3, 2):
            for way in (0, 1):
                pl.semaphore_signal(barrier, inc=1, device_id=at.device(*at.ring(way, step)), device_id_type=MESH)
        pl.semaphore_wait(barrier, 6)
        groups = [(way, first, second) for first in LATE for second in FAR_FIRST for way in (0, 1)]
        for which in groups:
            hop(*which).start()
        for which in groups:
            hop(*which).wait()


def piece(at, src, dst, sems, way, first, second):
    here = (at.place(*at.both(way, -first, -second)), at.rows(way))
    return pltpu.make_async_copy(src.at[here], dst.at[here], sems.at[(way * 4 + first) * 4 + second])


def write_early(key_in, value_in, high_in, low_in, key_out, value_out, high_out, low_out, done, sems):
    at = layout(key_in.shape[1])
    done[...] = jnp.zeros_like(done)
    copies = [
        pltpu.make_async_copy(key_in.at[pl.ds(4 * part, 4)], key_out.at[pl.ds(4 * part, 4)], sems.at[32 + part])
        for part in range(4)
    ]
    copies.append(pltpu.make_async_copy(high_in, high_out, sems.at[36]))
    copies.append(pltpu.make_async_copy(low_in, low_out, sems.at[37]))
    for copy in copies:
        copy.start()

    def each(first, seconds, act):
        for second in seconds:
            for way in (0, 1):
                act(piece(at, value_in, value_out, sems, way, first, second))

    for act in (lambda copy: copy.start(), lambda copy: copy.wait()):
        for first in GROUPS:
            each(first, (0,), act)
            at.on_late(first, False, lambda: each(first, FAR_FIRST, act))
    for copy in copies:
        copy.wait()


def write_late(_, value_in, value_out, sems):
    at = layout(value_in.shape[1])

    def each(first, act):
        for second in FAR_FIRST:
            for way in (0, 1):
                act(piece(at, value_in, value_out, sems, way, first, second))

    for act in (lambda copy: copy.start(), lambda copy: copy.wait()):
        for first in GROUPS:
            at.on_late(first, True, lambda: each(first, act))


def on_device(fresh_keys, fresh_values, turn_angle):
    batch, length, _, size = fresh_keys.shape
    half_head = turn_angle.shape[1]
    pages = batch * length // PAGE
    vmem, any_space = pl.BlockSpec(memory_space=pltpu.VMEM), pl.BlockSpec(memory_space=pl.ANY)
    whole, bounds = (batch, length, size), (pages, size)
    relay = (SIDE - 1, length // 2, size)
    early_keys, early_values, value_relay, high, low = pl.pallas_call(
        exchange,
        out_shape=(
            pltpu.VMEM(whole, jnp.bfloat16),
            pltpu.VMEM(whole, jnp.bfloat16),
            pltpu.VMEM((2, SIDE) + relay, jnp.bfloat16),
            pltpu.VMEM(bounds, jnp.bfloat16),
            pltpu.VMEM(bounds, jnp.bfloat16),
        ),
        in_specs=[any_space] * 3,
        out_specs=(vmem,) * 5,
        scratch_shapes=[
            pltpu.VMEM(whole, jnp.bfloat16),
            pltpu.VMEM(whole, jnp.bfloat16),
            pltpu.VMEM((2, SIDE - 1) + relay, jnp.bfloat16),
            pltpu.VMEM(bounds, jnp.float32),
            pltpu.VMEM(bounds, jnp.float32),
            pltpu.VMEM((half_head, length), jnp.float32),
            pltpu.VMEM((length, size), jnp.float32),
            pltpu.VMEM((length, size), jnp.float32),
            pltpu.SemaphoreType.DMA((128,)),
            pltpu.SemaphoreType.DMA((128,)),
            pltpu.SemaphoreType.DMA((16,)),
            pltpu.SemaphoreType.DMA((2,)),
            pltpu.SemaphoreType.DMA,
            pltpu.SemaphoreType.DMA((6,)),
            pltpu.SemaphoreType.REGULAR,
        ],
        compiler_params=pltpu.CompilerParams(
            collective_id=0, has_side_effects=True, vmem_limit_bytes=43 * 2**20
        ),
    )(fresh_keys.reshape(whole), fresh_values.reshape(whole), turn_angle.T)
    cache_keys, some_values, high, low, written = pl.pallas_call(
        write_early,
        out_shape=(
            jax.ShapeDtypeStruct(whole, jnp.bfloat16),
            jax.ShapeDtypeStruct(whole, jnp.bfloat16),
            jax.ShapeDtypeStruct(bounds, jnp.bfloat16),
            jax.ShapeDtypeStruct(bounds, jnp.bfloat16),
            pltpu.VMEM((8, size), jnp.float32),
        ),
        in_specs=[vmem] * 4,
        out_specs=(any_space,) * 4 + (vmem,),
        scratch_shapes=[pltpu.SemaphoreType.DMA((38,))],
        compiler_params=pltpu.CompilerParams(vmem_limit_bytes=2**20),
    )(early_keys, early_values, high, low)
    late_values = pl.pallas_call(
        last_groups,
        out_shape=pltpu.VMEM(whole, jnp.bfloat16),
        in_specs=[vmem] * 2,
        out_specs=vmem,
        scratch_shapes=[pltpu.SemaphoreType.DMA((32,)), pltpu.SemaphoreType.DMA((32,))],
        compiler_params=pltpu.CompilerParams(
            collective_id=1, has_side_effects=True, vmem_limit_bytes=4 * 2**20
        ),
    )(value_relay, written)
    cache_values = pl.pallas_call(
        write_late,
        out_shape=jax.ShapeDtypeStruct(whole, jnp.bfloat16),
        in_specs=[any_space, vmem],
        out_specs=any_space,
        input_output_aliases={0: 0},
        scratch_shapes=[pltpu.SemaphoreType.DMA((32,))],
        compiler_params=pltpu.CompilerParams(vmem_limit_bytes=2**20),
    )(some_values, late_values)
    return (
        cache_keys.reshape(1, -1, 1, size),
        cache_values.reshape(1, -1, 1, size),
        high.reshape(1, -1, 1, size),
        low.reshape(1, -1, 1, size),
    )


def solution(mesh):
    cut = P(None, ("coarse", "fine"), "model", None)
    whole = P(("coarse", "fine"), None, "model", None)
    return jax.shard_map(
        on_device, mesh=mesh, in_specs=(cut, cut, P()), out_specs=(whole,) * 4, check_vma=False
    )
```
